256 devices in a mesh: dp: 16 (over z, core), tensor: 16 (over y, x).
Axes of the slice: x: 4, y: 4, z: 8, core: 2. Of those that a mesh axis runs over, the one named last changes fastest.
Arguments:
- tokens: bfloat16 [4096, 4096], P('dp', 'tensor'), may hold values from -6 to 6
- cotangent: bfloat16 [4096, 4096], P('dp', 'tensor'), may hold values from -6 to 6
- gate_weight: bfloat16 [4096, 14336], P('dp', 'tensor'), may hold values from -0.09375 to 0.09375
- up_weight: bfloat16 [4096, 14336], P('dp', 'tensor'), may hold values from -0.09375 to 0.09375
- down_weight: bfloat16 [14336, 4096], P('tensor', 'dp'), may hold values from -0.046875 to 0.046875
- counts: int32 [16], replicated, may hold values from 0 to 16, as said below
Outputs:
- outputs: bfloat16 [4096, 4096], P('dp', 'tensor')
- input_grads: bfloat16 [4096, 4096], P('dp', 'tensor')
The draws below stay inside these ranges and needn't reach their ends.
Inputs may be any that keep to these rules, and one draw needn't show every extreme that they name: counts[r] is the number of live 16-row blocks at the head of rank r's buffer; counts[r] + counts[(r + 8) % 16] = 16 for every rank r, some rank has 16 and some rank has 0.
All inputs are finite; a program needn't handle non-finite values.
Results may differ from the reference program's by a relative error of at most 0.005.
Values may be sent and summed in bfloat16 or wider, within the bound.
No kernel may reach another device: no remote copies, remote signals or barrier semaphores. Data moves between devices by JAX's collectives and lax.ppermute only.
A program may use at most 128 MiB of HBM per device.

```python
import jax
import jax.numpy as jnp
from jax import lax

D = 4096
FF = 14336
BLOCK = 16
CAP_BLK = 16
ROWS = 4096
N_DP = 16


def draw_counts(key, part):
    moves = jax.random.randint(jax.random.fold_in(key, 12), (N_DP // 2,), -(CAP_BLK // 2), CAP_BLK // 2 + 1).astype(jnp.int32)
    moves = moves.at[0].set(CAP_BLK // 2)
    values = CAP_BLK // 2 + jnp.concatenate([moves, -moves])
    return values.astype(jnp.int32)


def block_levels(stream_key, extent, shards, low, high):
    def one(axis_at, parts):
        draws = jax.random.uniform(jax.random.fold_in(jax.random.fold_in(stream_key, 6), axis_at), (parts,), jnp.float32, low / len(shards), high / len(shards))
        return jnp.repeat(jnp.exp(draws), extent[axis_at] // parts).reshape((-1,) + (1,) * (len(extent) - axis_at - 1))

    gain = one(*shards[0])
    for cut in shards[1:]:
        gain = gain * one(*cut)
    return gain


def gaussian(rng, extent, deviation, limit, pieces=(), kind=jnp.bfloat16):
    result = deviation * jax.random.normal(rng, extent, jnp.float32)
    if pieces:
        result = result * block_levels(rng, extent, pieces, -0.22, 0.18)
    return jnp.clip(result, -limit, limit).astype(kind)


def setup_inputs(seed: int = 0) -> dict:
    seeds = jax.random.split(jax.random.key(seed), 7)
    return {
        "tokens": gaussian(seeds[0], (ROWS, D), 1.0, 6.0, ((0, 16), (1, 16))),
        "cotangent": gaussian(seeds[1], (ROWS, D), 1.0, 6.0, ((0, 16), (1, 16))),
        "gate_weight": gaussian(seeds[2], (D, FF), D ** -0.5, 0.09375, ((0, 16), (1, 16))),
        "up_weight": gaussian(seeds[3], (D, FF), D ** -0.5, 0.09375, ((0, 16), (1, 16))),
        "down_weight": gaussian(seeds[4], (FF, D), FF ** -0.5, 0.046875, ((0, 16), (1, 16))),
        "counts": draw_counts(jax.random.fold_in(seeds[6], 71), 0),
    }


def transposed(left, right):
    return lax.dot_general(left, right, (((1,), (1,)), ((), ())), preferred_element_type=jnp.float32)


def reference(tokens, cotangent, gate_weight, up_weight, down_weight, counts):
    block_ids = jnp.arange(CAP_BLK, dtype=jnp.int32)
    live_blocks = (block_ids[None, :] < counts[:, None]).astype(jnp.float32)
    row_mask = jnp.repeat(live_blocks, BLOCK, axis=1).reshape(N_DP * CAP_BLK * BLOCK, 1)
    gate_pre = jnp.dot(tokens, gate_weight, preferred_element_type=jnp.float32)
    up_pre = jnp.dot(tokens, up_weight, preferred_element_type=jnp.float32)
    sigmoid_gate = jax.nn.sigmoid(gate_pre)
    activated = gate_pre * sigmoid_gate
    hidden = (activated * up_pre).astype(jnp.bfloat16)
    outputs = (row_mask * jnp.dot(hidden, down_weight, preferred_element_type=jnp.float32)).astype(jnp.bfloat16)
    grad_hidden = transposed(cotangent, down_weight)
    grad_gate = (grad_hidden * up_pre * sigmoid_gate * (1.0 + gate_pre * (1.0 - sigmoid_gate))).astype(jnp.bfloat16)
    grad_up = (grad_hidden * activated).astype(jnp.bfloat16)
    summed = transposed(grad_gate, gate_weight) + transposed(grad_up, up_weight)
    input_grads = (row_mask * summed).astype(jnp.bfloat16)
    return outputs, input_grads
```

```python
import math

import jax
import jax.numpy as jnp
from jax import lax
from jax.experimental import pallas as pl
from jax.experimental.pallas import tpu as pltpu
from jax.sharding import PartitionSpec as P


BLOCK = 16
SIDE = 4
RING = 8
FAR = 4
TILE = 256
NEAR = (0, 7, 1, 6, 2, 5, 3)
F32 = jnp.float32
BF16 = jnp.bfloat16


def ring(block, step):
    route = [(((d // 2 - step) % RING) * 2 + d % 2, d) for d in range(2 * RING)]
    return lax.ppermute(block, "dp", route)


def swap(block):
    return lax.ppermute(block, "dp", [(d, d ^ 1) for d in range(2 * RING)])


def opposite(block):
    n = 2 * RING
    return lax.ppermute(block, "dp", [((d + n // 2) % n, d) for d in range(n)])


def dot(left, right):
    return jnp.dot(left, right, preferred_element_type=F32)


def size(shape, dtype):
    return math.prod(shape) * jnp.dtype(dtype).itemsize


def call(body, outs, scalars, *arrays):
    specs = [pl.BlockSpec(memory_space=pltpu.SMEM)]
    specs += [pl.BlockSpec(memory_space=pltpu.VMEM)] * len(arrays)
    held = sum(size(a.shape, a.dtype) for a in arrays) + sum(size(*o) for o in outs)
    return pl.pallas_call(
        body,
        out_shape=[jax.ShapeDtypeStruct(s, d) for s, d in outs],
        in_specs=specs,
        out_specs=[pl.BlockSpec(memory_space=pltpu.VMEM)] * len(outs),
        compiler_params=pltpu.CompilerParams(vmem_limit_bytes=held + (4 << 20)),
    )(scalars, *arrays)


CORE, SLOT, CHIP = 0, 1, 1 + RING


def arrange_features(table, mine, other, x_out, dy_out):
    rows = mine.shape[3]
    for core in range(2):

        @pl.when(table[CORE] == core)
        def _():
            at, away = core * rows, (1 - core) * rows
            for k in range(RING):
                slot = table[SLOT + k]
                for which, out in ((0, x_out), (1, dy_out)):
                    out[k, :, at : at + rows] = mine[slot, which]
                    out[k, :, away : away + rows] = other[slot, which]


def tiles(extent, size):
    return [(at, min(at + size, extent)) for at in range(0, extent, size)]


def gate_up_kernel(table, x, *refs):
    gates, ups, out = refs[:RING], refs[RING : 2 * RING], refs[2 * RING]
    for which, weights in ((0, gates), (1, ups)):
        for lo, hi in tiles(out.shape[1], TILE):
            out[which, lo:hi] = sum(dot(weights[k][lo:hi], x[k]) for k in range(RING))


def grad_hidden_kernel(table, dy, *refs):
    downs, out = refs[:-1], refs[-1]
    for lo, hi in tiles(out.shape[0], TILE):
        out[lo:hi] = sum(dot(downs[n][lo:hi], dy[k]) for n, k in enumerate(NEAR))


def grad_hidden_far(table, dy, near, far_a, far_b, out):
    cut = far_a.shape[0]
    out[:cut] = near[:cut] + dot(far_a[...], dy[FAR])
    out[cut:] = near[cut:] + dot(far_b[...], dy[FAR])


def keep_and_give(table, k, block, keep, give):
    rows = keep.shape[1]

    @pl.when(table[CORE] == 0)
    def _():
        keep[k] = block[:rows]
        give[k] = block[rows:]

    @pl.when(table[CORE] != 0)
    def _():
        keep[k] = block[rows:]
        give[k] = block[:rows]


def outputs_kernel(table, hidden_t, far_a, far_b, *refs):
    downs, (keep, give, hidden) = refs[:-3], refs[-3:]
    cut = far_a.shape[0]
    hidden[...] = hidden_t[...].T
    for n, k in enumerate(NEAR):
        keep_and_give(table, k, dot(hidden[...], downs[n][...]).astype(BF16), keep, give)
    far = dot(hidden[:, :cut], far_a[...]) + dot(hidden[:, cut:], far_b[...])
    keep_and_give(table, FAR, far.astype(BF16), keep, give)


def input_grads_kernel(table, mine, other, by_gate, by_up, *refs):
    gates, ups = refs[:RING], refs[RING : 2 * RING]
    keep, give, gg, gu = refs[2 * RING :]
    for lo, hi in tiles(mine.shape[0], TILE):
        grad_hidden = mine[lo:hi] + other[lo:hi]
        gg[:, lo:hi] = (grad_hidden * by_gate[lo:hi]).astype(BF16).T
        gu[:, lo:hi] = (grad_hidden * by_up[lo:hi]).astype(BF16).T
    for k in range(RING):
        block = dot(gg[...], gates[k][...]) + dot(gu[...], ups[k][...])
        keep_and_give(table, k, block.astype(BF16), keep, give)


def arrange_columns(table, mine, other, out):
    for s in range(2 * RING):
        k = (s // 2 - table[CHIP] + RING) % RING

        @pl.when(table[CORE] == s % 2)
        def _():
            out[s] = mine[k]

        @pl.when(table[CORE] != s % 2)
        def _():
            out[s] = other[k]


def per_device(tokens, cotangent, gate_weight, up_weight, down_weight, counts):
    rank = lax.axis_index("dp")
    z, c = rank // 2, rank % 2

    def around(own, after=None):
        right, left = [own], [own]
        for n in range(3):
            next_r, next_l = right[-1], left[-1]
            if n == 1 and after:
                next_r, _ = lax.optimization_barrier((next_r, after[0]))
                next_l, _ = lax.optimization_barrier((next_l, after[1]))
            right.append(ring(next_r, 1))
            left.append(ring(next_l, -1))
        return right, left

    g_r, g_l = around(gate_weight.T)
    u_r, u_l = around(up_weight.T)
    g_far, u_far = ring(g_r[3], 1), ring(u_l[3], -1)
    d_r, d_l = around(down_weight, (g_r[3], g_l[3]))
    cut = 512
    d_far = (ring(d_r[3][:cut], 1), ring(d_l[3][cut:], -1))

    def by_delta(r, l, far):
        return [r[0], l[1], l[2], l[3], far, r[3], r[2], r[1]]

    gates = by_delta(g_r, g_l, g_far)
    ups = by_delta(u_r, u_l, u_far)
    downs = by_delta(d_r, d_l, None)
    near_downs = [downs[k] for k in NEAR]

    rank_count = lax.axis_size("dp")
    blocks = tokens.shape[0] // BLOCK
    columns = tokens.shape[1]
    own_blocks = counts[rank]
    share = blocks // 2
    rows = share * BLOCK
    partner_count = counts[(rank + rank_count // 2) % rank_count]
    got = opposite(jnp.stack([tokens[rows:], cotangent[rows:]]))
    keep_blocks = jnp.minimum(own_blocks, share)
    slot_ids = jnp.arange(share, dtype=jnp.int32)
    foreign = slot_ids - own_blocks
    mine = slot_ids < keep_blocks
    valid = mine | (foreign >= 0) & (foreign < partner_count - share)
    source_index = jnp.where(mine, slot_ids, share + jnp.clip(foreign, 0, share - 1))
    lower = jnp.stack([tokens[:rows], cotangent[:rows]])
    stacked = jnp.concatenate([lower.reshape(2, share, BLOCK, columns), got.reshape(2, share, BLOCK, columns)], axis=1)
    pieces = jnp.take(stacked, source_index, axis=1)
    pieces = jnp.where(valid[None, :, None, None], pieces, jnp.zeros_like(pieces))
    work = pieces.reshape(2, rows, columns).transpose(0, 2, 1)
    live_rows = jnp.repeat(valid.astype(F32), BLOCK)[:, None]

    spread = jnp.broadcast_to(work[None], (SIDE * SIDE, *work.shape))
    every = lax.all_to_all(spread, "tensor", 0, 0, tiled=True)
    slots = 2 * ((z + jnp.arange(RING, dtype=jnp.int32)) % RING) + c
    every_other = swap(every)
    table = jnp.concatenate([c[None], slots, z[None]]).astype(jnp.int32)
    wide = (RING, columns, 2 * rows)
    x_all, dy_all = call(arrange_features, [(wide, BF16)] * 2, table, every, every_other)

    ff = gate_weight.shape[1]
    by_row = (ff, 2 * rows)
    turned = ((2 * rows, ff), BF16)
    parts = call(gate_up_kernel, [((2,) + by_row, F32)], table, x_all, *gates, *ups)[0]
    sums = parts + swap(parts)
    gate_pre, up_pre = sums[0], sums[1]
    sigmoid_gate = jax.nn.sigmoid(gate_pre)
    activated = gate_pre * sigmoid_gate
    hidden = (activated * up_pre).astype(BF16)
    by_gate = up_pre * sigmoid_gate * (1.0 + gate_pre * (1.0 - sigmoid_gate))

    half = ((RING, rows, columns), BF16)

    def reduce_columns(keep, give):
        share_of = ((2 * RING, rows, columns), BF16)
        blocks_for = call(arrange_columns, [share_of], table, keep, swap(give))[0]
        got_blocks = lax.all_to_all(blocks_for, "tensor", 0, 0, tiled=True)
        return jnp.sum(got_blocks.astype(F32), axis=0)

    grad_near = call(grad_hidden_kernel, [(by_row, F32)], table, dy_all, *near_downs)[0]
    grad_part = call(grad_hidden_far, [(by_row, F32)], table, dy_all, grad_near, *d_far)[0]
    grad_other = swap(grad_part)
    out = call(outputs_kernel, [half, half, turned], table, hidden, *d_far, *near_downs)
    out_sum = reduce_columns(out[0], out[1])
    dx = call(input_grads_kernel, [half, half, turned, turned], table, grad_part, grad_other, by_gate, activated, *gates, *ups)
    dx_sum = reduce_columns(dx[0], dx[1])

    back_pos = own_blocks + slot_ids
    back_ok = back_pos < share
    back_index = jnp.clip(back_pos, 0, share - 1)
    upper_live = slot_ids < own_blocks - share

    done = (jnp.stack([out_sum, dx_sum]) * live_rows).astype(BF16).reshape(2, share, BLOCK, columns)
    back = jnp.take(done, back_index, axis=1)
    back = jnp.where(back_ok[:, None, None], back, jnp.zeros_like(back))
    returned = opposite(back)
    low = jnp.where(mine[:, None, None], done, jnp.zeros_like(done))
    high = jnp.where(upper_live[:, None, None], returned, jnp.zeros_like(returned))
    home = jnp.concatenate([low, high], axis=1).reshape(2, 2 * rows, columns)
    return home[0], home[1]


def solution(mesh):
    in_specs = (
        P("dp", "tensor"),
        P("dp", "tensor"),
        P("dp", "tensor"),
        P("dp", "tensor"),
        P("tensor", "dp"),
        P(),
    )
    out_specs = (P("dp", "tensor"), P("dp", "tensor"))

    return jax.shard_map(per_device, mesh=mesh, in_specs=in_specs, out_specs=out_specs, check_vma=False)
```

```python
import math

import jax
import jax.numpy as jnp
from jax import lax
from jax.experimental import pallas as pl
from jax.experimental.pallas import tpu as pltpu
from jax.sharding import PartitionSpec as P


BLOCK = 16
SIDE = 4
RING = 8
FAR = 4
TILE = 256
CUT = 512
SPLIT = (5, 3)
NEAR = (0, 7, 1, 6, 2, 5, 3)
F32 = jnp.float32
BF16 = jnp.bfloat16


def ring(block, step):
    route = [(((d // 2 - step) % RING) * 2 + d % 2, d) for d in range(2 * RING)]
    return lax.ppermute(block, "dp", route)


def swap(block):
    return lax.ppermute(block, "dp", [(d, d ^ 1) for d in range(2 * RING)])


def opposite(block):
    n = 2 * RING
    return lax.ppermute(block, "dp", [((d + n // 2) % n, d) for d in range(n)])


def dot(left, right):
    return jnp.dot(left, right, preferred_element_type=F32)


def size(shape, dtype):
    return math.prod(shape) * jnp.dtype(dtype).itemsize


def call(body, outs, scalars, *arrays, loaded=(), scratch=(), aliases=None):
    specs = [pl.BlockSpec(memory_space=pltpu.SMEM)]
    specs += [pl.BlockSpec(memory_space=pltpu.VMEM)] * len(arrays)
    specs += [pl.BlockSpec(memory_space=pl.ANY)] * len(loaded)
    held = sum(size(a.shape, a.dtype) for a in arrays + tuple(loaded)) + sum(size(*o) for o in outs)
    return pl.pallas_call(
        body,
        out_shape=[jax.ShapeDtypeStruct(s, d) for s, d in outs],
        in_specs=specs,
        out_specs=[pl.BlockSpec(memory_space=pl.ANY if aliases else pltpu.VMEM)] * len(outs),
        scratch_shapes=list(scratch),
        input_output_aliases=aliases or {},
        compiler_params=pltpu.CompilerParams(vmem_limit_bytes=held + (6 << 20)),
    )(scalars, *arrays, *loaded)


CORE, SLOT, CHIP = 0, 1, 1 + RING


def arrange_features(table, mine, other, x_out, dy_out):
    rows = mine.shape[3]
    for core in range(2):

        @pl.when(table[CORE] == core)
        def _():
            at, away = core * rows, (1 - core) * rows
            for k in range(RING):
                slot = table[SLOT + k]
                for which, out in ((0, x_out), (1, dy_out)):
                    out[k, :, at : at + rows] = mine[slot, which]
                    out[k, :, away : away + rows] = other[slot, which]


def tiles(extent, size):
    return [(at, min(at + size, extent)) for at in range(0, extent, size)]


def gate_up_kernel(table, x, *refs):
    gates, ups, out = refs[:RING], refs[RING : 2 * RING], refs[2 * RING]
    for which, weights in ((0, gates), (1, ups)):
        for lo, hi in tiles(out.shape[1], TILE):
            out[which, lo:hi] = sum(dot(weights[k][lo:hi], x[k]) for k in range(RING))


def pieces_of(refs, split):
    refs, found = list(refs), {}
    for k in NEAR:
        if k in split:
            low, high = refs.pop(0), refs.pop(0)
            found[k] = [(0, CUT, low), (CUT, CUT + high.shape[0], high)]
        else:
            ref = refs.pop(0)
            found[k] = [(0, ref.shape[0], ref)]
    return found


def rows_of(parts, lo, hi):
    for at, end, ref in parts:
        if at <= lo and hi <= end:
            return ref[lo - at : hi - at]


def grad_hidden_kernel(table, dy, *refs):
    downs, out = pieces_of(refs[:-1], SPLIT), refs[-1]
    for lo, hi in tiles(out.shape[0], TILE):
        out[lo:hi] = sum(dot(rows_of(downs[k], lo, hi), dy[k]) for k in NEAR)


def grad_hidden_far(table, dy, near, far_a, far_b, out):
    out[:CUT] = near[:CUT] + dot(far_a[...], dy[FAR])
    out[CUT:] = near[CUT:] + dot(far_b[...], dy[FAR])


def keep_and_give(table, k, block, keep, give):
    rows = keep.shape[1]

    @pl.when(table[CORE] == 0)
    def _():
        keep[k] = block[:rows]
        give[k] = block[rows:]

    @pl.when(table[CORE] != 0)
    def _():
        keep[k] = block[rows:]
        give[k] = block[:rows]


def outputs_near(table, hidden_t, *refs):
    downs, (keep, give, hidden) = pieces_of(refs[:-3], SPLIT), refs[-3:]
    hidden[...] = hidden_t[...].T
    for k in NEAR:
        block = sum(dot(hidden[:, lo:hi], ref[...]) for lo, hi, ref in downs[k])
        keep_and_give(table, k, block.astype(BF16), keep, give)


def outputs_far(table, hidden, far_a, far_b, keep_in, give_in, keep, give, block, sems):
    far = dot(hidden[:, :CUT], far_a[...]) + dot(hidden[:, CUT:], far_b[...])
    far = far.astype(BF16)
    keep_and_give(table, 0, far, block.at[0:1], block.at[1:2])
    copies = [pltpu.make_async_copy(block.at[i], out.at[FAR], sems.at[i]) for i, out in enumerate((keep, give))]
    for copy in copies:
        copy.start()
    for copy in copies:
        copy.wait()


def input_grads_kernel(table, mine, other, by_gate, by_up, *refs):
    weights, (keep, give, gg, gu, held, sems) = refs[: 2 * RING], refs[2 * RING :]
    copies = []
    for n in range(RING):
        for i in (n, RING + n):
            copies.append(pltpu.make_async_copy(weights[i], held.at[i], sems.at[i]))
            copies[-1].start()
    for lo, hi in tiles(mine.shape[0], TILE):
        grad_hidden = mine[lo:hi] + other[lo:hi]
        gg[:, lo:hi] = (grad_hidden * by_gate[lo:hi]).astype(BF16).T
        gu[:, lo:hi] = (grad_hidden * by_up[lo:hi]).astype(BF16).T
    for k in range(RING):
        copies[2 * k].wait()
        copies[2 * k + 1].wait()
        block = dot(gg[...], held[k]) + dot(gu[...], held[RING + k])
        keep_and_give(table, k, block.astype(BF16), keep, give)


def arrange_columns(table, mine, other, out):
    for s in range(2 * RING):
        k = (s // 2 - table[CHIP] + RING) % RING

        @pl.when(table[CORE] == s % 2)
        def _():
            out[s] = mine[k]

        @pl.when(table[CORE] != s % 2)
        def _():
            out[s] = other[k]


def per_device(tokens, cotangent, gate_weight, up_weight, down_weight, counts):
    rank = lax.axis_index("dp")
    z, c = rank // 2, rank % 2

    def around(own, hops):
        right, left = [own], [own]
        for _ in range(hops):
            right.append(ring(right[-1], 1))
            left.append(ring(left[-1], -1))
        return right, left

    g_r, g_l = around(gate_weight.T, 3)
    u_r, u_l = around(up_weight.T, 3)
    d_r, d_l = around(down_weight, 2)
    g_far = ring(g_r[3], 1)
    u_far = ring(u_l[3], -1)
    d_r3a = ring(d_r[2][:CUT], 1)
    d_l3b = ring(d_l[2][CUT:], -1)
    d_r3b = ring(d_r[2][CUT:], 1)
    d_l3a = ring(d_l[2][:CUT], -1)
    d_far = (ring(d_r3a, 1), ring(d_l3b, -1))

    def by_delta(r, l, far):
        return [r[0], l[1], l[2], l[3], far, r[3], r[2], r[1]]

    gates = by_delta(g_r, g_l, g_far)
    ups = by_delta(u_r, u_l, u_far)
    downs = {0: [down_weight], 7: [d_r[1]], 1: [d_l[1]], 6: [d_r[2]], 2: [d_l[2]], 5: [d_r3a, d_r3b], 3: [d_l3a, d_l3b]}
    near_downs = [piece for k in NEAR for piece in downs[k]]

    rank_count = lax.axis_size("dp")
    blocks = tokens.shape[0] // BLOCK
    columns = tokens.shape[1]
    own_blocks = counts[rank]
    share = blocks // 2
    rows = share * BLOCK
    partner_count = counts[(rank + rank_count // 2) % rank_count]
    got = opposite(jnp.stack([tokens[rows:], cotangent[rows:]]))
    keep_blocks = jnp.minimum(own_blocks, share)
    slot_ids = jnp.arange(share, dtype=jnp.int32)
    foreign = slot_ids - own_blocks
    mine = slot_ids < keep_blocks
    valid = mine | (foreign >= 0) & (foreign < partner_count - share)
    source_index = jnp.where(mine, slot_ids, share + jnp.clip(foreign, 0, share - 1))
    lower = jnp.stack([tokens[:rows], cotangent[:rows]])
    stacked = jnp.concatenate([lower.reshape(2, share, BLOCK, columns), got.reshape(2, share, BLOCK, columns)], axis=1)
    pieces = jnp.take(stacked, source_index, axis=1)
    pieces = jnp.where(valid[None, :, None, None], pieces, jnp.zeros_like(pieces))
    work = pieces.reshape(2, rows, columns).transpose(0, 2, 1)
    live_rows = jnp.repeat(valid.astype(F32), BLOCK)[:, None]

    spread = jnp.broadcast_to(work[None], (SIDE * SIDE, *work.shape))
    every = lax.all_to_all(spread, "tensor", 0, 0, tiled=True)
    slots = 2 * ((z + jnp.arange(RING, dtype=jnp.int32)) % RING) + c
    every_other = swap(every)
    table = jnp.concatenate([c[None], slots, z[None]]).astype(jnp.int32)
    wide = (RING, columns, 2 * rows)
    x_all, dy_all = call(arrange_features, [(wide, BF16)] * 2, table, every, every_other)

    ff = gate_weight.shape[1]
    by_row = (ff, 2 * rows)
    turned = ((2 * rows, ff), BF16)
    parts = call(gate_up_kernel, [((2,) + by_row, F32)], table, x_all, *gates, *ups)[0]
    parts_other = swap(parts)
    sums = parts + parts_other
    gate_pre, up_pre = sums[0], sums[1]
    sigmoid_gate = jax.nn.sigmoid(gate_pre)
    activated = gate_pre * sigmoid_gate
    hidden = (activated * up_pre).astype(BF16)
    by_gate = up_pre * sigmoid_gate * (1.0 + gate_pre * (1.0 - sigmoid_gate))

    half = ((RING, rows, columns), BF16)

    def reduce_columns(keep, give):
        share_of = ((2 * RING, rows, columns), BF16)
        got_cols = swap(give)
        blocks_for = call(arrange_columns, [share_of], table, keep, got_cols)[0]
        got_blocks = lax.all_to_all(blocks_for, "tensor", 0, 0, tiled=True)
        return jnp.sum(got_blocks.astype(F32), axis=0)

    grad_near = call(grad_hidden_kernel, [(by_row, F32)], table, dy_all, *near_downs)[0]
    out_near = call(outputs_near, [half, half, turned], table, hidden, *near_downs)
    grad_part = call(grad_hidden_far, [(by_row, F32)], table, dy_all, grad_near, *d_far)[0]
    grad_other = swap(grad_part)
    out = call(
        outputs_far, [half, half], table, out_near[2], *d_far, loaded=out_near[:2],
        scratch=[pltpu.VMEM((2, rows, columns), BF16), pltpu.SemaphoreType.DMA((2,))], aliases={4: 0, 5: 1},
    )
    out_sum = reduce_columns(*out)
    scratch = [pltpu.VMEM(*turned), pltpu.VMEM(*turned)]
    scratch += [pltpu.VMEM((2 * RING, ff, columns), BF16), pltpu.SemaphoreType.DMA((2 * RING,))]
    dx = call(
        input_grads_kernel, [half, half], table, grad_part, grad_other, by_gate, activated,
        loaded=gates + ups, scratch=scratch,
    )
    dx_sum = reduce_columns(*dx)

    back_pos = own_blocks + slot_ids
    back_ok = back_pos < share
    back_index = jnp.clip(back_pos, 0, share - 1)
    upper_live = slot_ids < own_blocks - share

    done = (jnp.stack([out_sum, dx_sum]) * live_rows).astype(BF16).reshape(2, share, BLOCK, columns)
    back = jnp.take(done, back_index, axis=1)
    back = jnp.where(back_ok[:, None, None], back, jnp.zeros_like(back))
    returned = opposite(back)
    low = jnp.where(mine[:, None, None], done, jnp.zeros_like(done))
    high = jnp.where(upper_live[:, None, None], returned, jnp.zeros_like(returned))
    home = jnp.concatenate([low, high], axis=1).reshape(2, 2 * rows, columns)
    return home[0], home[1]


def solution(mesh):
    in_specs = (
        P("dp", "tensor"),
        P("dp", "tensor"),
        P("dp", "tensor"),
        P("dp", "tensor"),
        P("tensor", "dp"),
        P(),
    )
    out_specs = (P("dp", "tensor"), P("dp", "tensor"))

    return jax.shard_map(per_device, mesh=mesh, in_specs=in_specs, out_specs=out_specs, check_vma=False)
```

```python
import functools
import math

import jax
import jax.numpy as jnp
from jax import lax
from jax.experimental import pallas as pl
from jax.experimental.pallas import tpu as pltpu
from jax.sharding import PartitionSpec as P


BLOCK = 16
SIDE = 4
RING = 8
TILE = 256
ARRIVAL = (0, 7, 1, 6, 2, 5, 3, 4)
NEAR = RING - 1
EARLY = 5
F32 = jnp.float32
BF16 = jnp.bfloat16


def ring(block, step):
    route = [(((d // 2 - step) % RING) * 2 + d % 2, d) for d in range(2 * RING)]
    return lax.ppermute(block, "dp", route)


def swap(block):
    return lax.ppermute(block, "dp", [(d, d ^ 1) for d in range(2 * RING)])


def opposite(block):
    n = 2 * RING
    return lax.ppermute(block, "dp", [((d + n // 2) % n, d) for d in range(n)])


def dot(left, right):
    return jnp.dot(left, right, preferred_element_type=F32)


def dot_t(left, right):
    return lax.dot_general(left, right, (((1,), (1,)), ((), ())), preferred_element_type=F32)


def size(shape, dtype):
    return math.prod(shape) * jnp.dtype(dtype).itemsize


def call(body, outs, scalars, *arrays, loaded=(), scratch=(), aliases=None):
    specs = [pl.BlockSpec(memory_space=pltpu.SMEM)]
    specs += [pl.BlockSpec(memory_space=pltpu.VMEM)] * len(arrays)
    specs += [pl.BlockSpec(memory_space=pl.ANY)] * len(loaded)
    held = sum(size(a.shape, a.dtype) for a in arrays) + sum(size(*o) for o in outs)
    return pl.pallas_call(
        body,
        out_shape=[jax.ShapeDtypeStruct(s, d) for s, d in outs],
        in_specs=specs,
        out_specs=[pl.BlockSpec(memory_space=pl.ANY if aliases else pltpu.VMEM)] * len(outs),
        scratch_shapes=list(scratch),
        input_output_aliases=aliases or {},
        compiler_params=pltpu.CompilerParams(vmem_limit_bytes=held + (6 << 20) + (8 << 20 if len(loaded) > RING else 0)),
    )(scalars, *arrays, *loaded)


CORE, SLOT, PLACE = 0, 1, 1 + RING


def loop(count, body):
    lax.fori_loop(0, count, lambda i, carry: (body(i), carry)[1], 0)


def tile_loop(extent, body):
    full = extent // TILE
    loop(full, lambda i: body(pl.ds(pl.multiple_of(i * TILE, TILE), TILE)))
    if extent % TILE:
        body(slice(full * TILE, extent))


def arrange_features(table, mine, other, x_out, dy_out):
    rows = mine.shape[2]
    at = pl.multiple_of(table[CORE] * rows, rows)
    away = pl.multiple_of((1 - table[CORE]) * rows, rows)

    def one(n):
        slot = table[SLOT + n]
        for which, out in ((0, x_out), (1, dy_out)):
            out[n, pl.ds(at, rows), :] = mine[slot, which]
            out[n, pl.ds(away, rows), :] = other[slot, which]

    loop(RING, one)


def fetch(refs, held, sems):
    copies = [pltpu.make_async_copy(ref, held.at[i], sems.at[i]) for i, ref in enumerate(refs)]
    for copy in copies:
        copy.start()


def fetched(held, sems, i):
    pltpu.make_async_copy(held.at[i], held.at[i], sems.at[i]).wait()


def early_sums(table, x, *refs, turned):
    weights, (out, held, sems) = refs[:-3], refs[-3:]
    fetch(weights, held, sems)
    loop(EARLY, lambda i: fetched(held, sems, i))

    def tile(part):
        if turned:
            out[:, part] = sum(dot_t(x[n], held[n, part, :]) for n in range(EARLY))
        else:
            out[:, part] = sum(dot(x[n], held[n, :, part]) for n in range(EARLY))

    tile_loop(out.shape[1], tile)


def gate_up_late(table, x, gate_early, up_early, *refs):
    weights, (out, give, held, sems) = refs[:-4], refs[-4:]
    late = RING - EARLY
    fetch(weights, held, sems)
    loop(2 * late, lambda i: fetched(held, sems, i))

    def tile(part):
        for which, early in enumerate((gate_early, up_early)):
            more = sum(dot_t(x[EARLY + n], held[which * late + n, part, :]) for n in range(late))
            total = early[:, part] + more
            out[which, :, part] = total
            give[which, :, part] = total.astype(BF16)

    tile_loop(out.shape[2], tile)


def grad_late(table, dy, early, *refs):
    downs, (out, held, sems) = refs[:-3], refs[-3:]
    late = NEAR - EARLY
    fetch(downs, held, sems)
    loop(late, lambda i: fetched(held, sems, i))

    def tile(part):
        out[:, part] = early[:, part] + sum(dot(dy[EARLY + n], held[n, :, part]) for n in range(late))

    tile_loop(out.shape[1], tile)


def grad_hidden_far(table, dy, near, far, out):
    def tile(part):
        out[:, part] = near[:, part] + dot(dy[NEAR], far[:, part])

    tile_loop(out.shape[1], tile)


def keep_and_give(table, n, block, both, keep, give):
    rows = keep.shape[1]
    both[...] = block.astype(BF16)
    keep[n] = both[pl.ds(pl.multiple_of(table[CORE] * rows, rows), rows), :]
    give[n] = both[pl.ds(pl.multiple_of((1 - table[CORE]) * rows, rows), rows), :]


def outputs_kernel(table, mine, other, early, late, far, keep, give, hidden, both):
    def tile(part):
        gate_pre = mine[0, :, part] + other[0, :, part].astype(F32)
        up_pre = mine[1, :, part] + other[1, :, part].astype(F32)
        activated = gate_pre * jax.nn.sigmoid(gate_pre)
        hidden[:, part] = (activated * up_pre).astype(BF16)

    tile_loop(hidden.shape[1], tile)
    loop(EARLY, lambda n: keep_and_give(table, n, dot_t(hidden[...], early[n]), both, keep, give))
    more = NEAR - EARLY
    loop(more, lambda n: keep_and_give(table, EARLY + n, dot_t(hidden[...], late[n]), both, keep, give))
    keep_and_give(table, NEAR, dot_t(hidden[...], far[...]), both, keep, give)


def input_grads_kernel(table, mine, other, by_gate, by_up, *refs):
    weights, (keep, give, gg, gu, both, held, sems) = refs[: 2 * RING], refs[2 * RING :]
    fetch(weights, held, sems)

    def tile(part):
        grad_hidden = mine[:, part] + other[:, part]
        gg[:, part] = (grad_hidden * by_gate[:, part]).astype(BF16)
        gu[:, part] = (grad_hidden * by_up[:, part]).astype(BF16)

    tile_loop(mine.shape[1], tile)

    def one(n):
        fetched(held, sems, 2 * n)
        fetched(held, sems, 2 * n + 1)
        keep_and_give(table, n, dot(gg[...], held[2 * n]) + dot(gu[...], held[2 * n + 1]), both, keep, give)

    loop(RING, one)


def arrange_columns(table, mine, other, out):
    def one(chip):
        place = table[PLACE + chip]
        out[2 * chip + table[CORE]] = mine[place]
        out[2 * chip + 1 - table[CORE]] = other[place]

    loop(RING, one)


def finish_kernel(table, got, done, back):
    share = done.shape[0]

    def add(j):
        part = pl.ds(pl.multiple_of(j * BLOCK, BLOCK), BLOCK)
        total = sum(got[s, part, :].astype(F32) for s in range(got.shape[0]))
        done[j] = jnp.where(table[j] != 0, total, 0.0).astype(BF16)

    def send(j):
        block = done[table[2 * share + j]].astype(F32)
        back[j] = jnp.where(table[share + j] != 0, block, 0.0).astype(BF16)

    loop(share, add)
    loop(share, send)


def per_device(tokens, cotangent, gate_weight, up_weight, down_weight, counts):
    rank = lax.axis_index("dp")
    z, c = rank // 2, rank % 2

    def around(own, hops):
        right, left = [own], [own]
        for _ in range(hops):
            right.append(ring(right[-1], 1))
            left.append(ring(left[-1], -1))
        return right, left

    g_r, g_l = around(gate_weight.T, 3)
    u_r, u_l = around(up_weight.T, 3)
    d_r, d_l = around(down_weight.T, 3)
    g_far = ring(g_r[3], 1)
    u_far = ring(u_l[3], -1)
    d_far = ring(d_l[3], -1)

    def near_of(r, l):
        slices = {0: r[0], 1: l[1], 2: l[2], 3: l[3], 5: r[3], 6: r[2], 7: r[1]}
        return [slices[k] for k in ARRIVAL[:-1]]

    rank_count = lax.axis_size("dp")
    blocks = tokens.shape[0] // BLOCK
    columns = tokens.shape[1]
    own_blocks = counts[rank]
    share = blocks // 2
    rows = share * BLOCK
    partner_count = counts[(rank + rank_count // 2) % rank_count]
    got = opposite(jnp.stack([tokens[rows:], cotangent[rows:]]))
    keep_blocks = jnp.minimum(own_blocks, share)
    slot_ids = jnp.arange(share, dtype=jnp.int32)
    foreign = slot_ids - own_blocks
    mine = slot_ids < keep_blocks
    valid = mine | (foreign >= 0) & (foreign < partner_count - share)
    source_index = jnp.where(mine, slot_ids, share + jnp.clip(foreign, 0, share - 1))
    lower = jnp.stack([tokens[:rows], cotangent[:rows]])
    stacked = jnp.concatenate([lower.reshape(2, share, BLOCK, columns), got.reshape(2, share, BLOCK, columns)], axis=1)
    pieces = jnp.take(stacked, source_index, axis=1)
    pieces = jnp.where(valid[None, :, None, None], pieces, jnp.zeros_like(pieces))
    work = pieces.reshape(2, rows, columns)

    spread = jnp.broadcast_to(work[None], (SIDE * SIDE, *work.shape))
    every = lax.all_to_all(spread, "tensor", 0, 0, tiled=True)
    slots = 2 * ((z + jnp.array(ARRIVAL, jnp.int32)) % RING) + c
    order = jnp.array([ARRIVAL.index(k) for k in range(RING)], jnp.int32)
    places = lax.dynamic_slice_in_dim(jnp.concatenate([order, order]), (RING - z) % RING, RING)
    every_other = swap(every)
    table = jnp.concatenate([c[None], slots, places]).astype(jnp.int32)
    wide = (RING, 2 * rows, columns)
    x_all, dy_all = call(arrange_features, [(wide, BF16)] * 2, table, every, every_other)

    ff = gate_weight.shape[1]
    by_row = (2 * rows, ff)

    def arrivals(count):
        return [pltpu.SemaphoreType.DMA((count,))]

    def early_of(x, slices, turned, keep=False):
        held = (EARLY, *slices[0].shape)
        return call(
            functools.partial(early_sums, turned=turned),
            [(by_row, F32)] + [(held, BF16)] * keep, table, x, loaded=slices[:EARLY],
            scratch=[pltpu.VMEM(held, BF16)] * (not keep) + arrivals(EARLY),
        )

    gate_all, up_all = near_of(g_r, g_l) + [g_far], near_of(u_r, u_l) + [u_far]
    gate_early = early_of(x_all, gate_all, True)[0]
    up_early = early_of(x_all, up_all, True)[0]
    late = RING - EARLY
    parts, parts_give = call(
        gate_up_late, [((2,) + by_row, F32), ((2,) + by_row, BF16)], table, x_all, gate_early, up_early,
        loaded=gate_all[EARLY:] + up_all[EARLY:],
        scratch=[pltpu.VMEM((2 * late, ff, columns), BF16)] + arrivals(2 * late),
    )
    parts_other = swap(parts_give)
    sums = parts + parts_other.astype(F32)
    gate_pre, up_pre = sums[0], sums[1]
    sigmoid_gate = jax.nn.sigmoid(gate_pre)
    activated = gate_pre * sigmoid_gate
    by_gate = up_pre * sigmoid_gate * (1.0 + gate_pre * (1.0 - sigmoid_gate))

    eight = ((RING, rows, columns), BF16)
    both = pltpu.VMEM((2 * rows, columns), BF16)

    def reduce_columns(keep, give):
        share_of = ((2 * RING, rows, columns), BF16)
        got_cols = swap(give)
        blocks_for = call(arrange_columns, [share_of], table, keep, got_cols)[0]
        return lax.all_to_all(blocks_for, "tensor", 0, 0, tiled=True)

    down_near = near_of(d_r, d_l)
    grad_early, down_early = early_of(dy_all, down_near, False, keep=True)
    grad_near, down_late = call(
        grad_late, [(by_row, F32), ((NEAR - EARLY, columns, ff), BF16)], table, dy_all, grad_early,
        loaded=down_near[EARLY:], scratch=arrivals(NEAR - EARLY),
    )
    grad_part = call(grad_hidden_far, [(by_row, F32)], table, dy_all, grad_near, d_far)[0]
    grad_other = swap(grad_part)
    out = call(
        outputs_kernel, [eight, eight], table, parts, parts_other, down_early, down_late, d_far,
        scratch=[pltpu.VMEM(by_row, BF16), both],
    )
    out_sum = reduce_columns(*out)
    pairs = zip(near_of(g_r, g_l) + [g_far], near_of(u_r, u_l) + [u_far])
    dx_weights = [w for pair in pairs for w in pair]
    scratch = [pltpu.VMEM(by_row, BF16)] * 2 + [both, pltpu.VMEM((2 * RING, ff, columns), BF16)] + arrivals(2 * RING)
    dx = call(
        input_grads_kernel, [eight, eight], table, grad_part, grad_other, by_gate, activated,
        loaded=dx_weights, scratch=scratch,
    )
    dx_sum = reduce_columns(*dx)

    back_pos = own_blocks + slot_ids
    back_ok = back_pos < share
    back_index = jnp.clip(back_pos, 0, share - 1)
    upper_live = slot_ids < own_blocks - share

    blocks_table = jnp.concatenate([valid, back_ok, back_index]).astype(jnp.int32)

    def home(got_blocks):
        eight_blocks = ((share, BLOCK, columns), BF16)
        done, back = call(finish_kernel, [eight_blocks] * 2, blocks_table, got_blocks)
        returned = opposite(back)
        low = jnp.where(mine[:, None, None], done, jnp.zeros_like(done))
        high = jnp.where(upper_live[:, None, None], returned, jnp.zeros_like(returned))
        return jnp.concatenate([low, high], axis=0).reshape(2 * rows, columns)

    return home(out_sum), home(dx_sum)


def solution(mesh):
    in_specs = (
        P("dp", "tensor"),
        P("dp", "tensor"),
        P("dp", "tensor"),
        P("dp", "tensor"),
        P("tensor", "dp"),
        P(),
    )
    out_specs = (P("dp", "tensor"), P("dp", "tensor"))

    return jax.shard_map(per_device, mesh=mesh, in_specs=in_specs, out_specs=out_specs, check_vma=False)
```

```python
import functools
import math

import jax
import jax.numpy as jnp
from jax import lax
from jax.experimental import pallas as pl
from jax.experimental.pallas import tpu as pltpu
from jax.sharding import PartitionSpec as P


BLOCK = 16
SIDE = 4
RING = 8
TILE = 256
ARRIVAL = (0, 7, 1, 6, 2, 5, 3, 4)
NEAR = RING - 1
EARLY = 5
F32 = jnp.float32
BF16 = jnp.bfloat16


def ring(block, step):
    route = [(((d // 2 - step) % RING) * 2 + d % 2, d) for d in range(2 * RING)]
    return lax.ppermute(block, "dp", route)


def swap(block):
    return lax.ppermute(block, "dp", [(d, d ^ 1) for d in range(2 * RING)])


def opposite(block):
    n = 2 * RING
    return lax.ppermute(block, "dp", [((d + n // 2) % n, d) for d in range(n)])


def dot(left, right):
    return jnp.dot(left, right, preferred_element_type=F32)


def dot_t(left, right):
    return lax.dot_general(left, right, (((1,), (1,)), ((), ())), preferred_element_type=F32)


def size(shape, dtype):
    return math.prod(shape) * jnp.dtype(dtype).itemsize


def call(body, outs, scalars, *arrays, loaded=(), scratch=(), aliases=None):
    specs = [pl.BlockSpec(memory_space=pltpu.SMEM)]
    specs += [pl.BlockSpec(memory_space=pltpu.VMEM)] * len(arrays)
    specs += [pl.BlockSpec(memory_space=pl.ANY)] * len(loaded)
    held = sum(size(a.shape, a.dtype) for a in arrays) + sum(size(*o) for o in outs)
    return pl.pallas_call(
        body,
        out_shape=[jax.ShapeDtypeStruct(s, d) for s, d in outs],
        in_specs=specs,
        out_specs=[pl.BlockSpec(memory_space=pl.ANY if aliases else pltpu.VMEM)] * len(outs),
        scratch_shapes=list(scratch),
        input_output_aliases=aliases or {},
        compiler_params=pltpu.CompilerParams(vmem_limit_bytes=held + (6 << 20) + (8 << 20 if len(loaded) > RING else 0)),
    )(scalars, *arrays, *loaded)


CORE, SLOT, PLACE = 0, 1, 1 + RING


def loop(count, body):
    lax.fori_loop(0, count, lambda i, carry: (body(i), carry)[1], 0)


def tile_loop(extent, body):
    full = extent // TILE
    loop(full, lambda i: body(pl.ds(pl.multiple_of(i * TILE, TILE), TILE)))
    if extent % TILE:
        body(slice(full * TILE, extent))


def arrange_features(table, mine, other, x_out, dy_out):
    rows = mine.shape[2]
    at = pl.multiple_of(table[CORE] * rows, rows)
    away = pl.multiple_of((1 - table[CORE]) * rows, rows)

    def one(n):
        slot = table[SLOT + n]
        for which, out in ((0, x_out), (1, dy_out)):
            out[n, pl.ds(at, rows), :] = mine[slot, which]
            out[n, pl.ds(away, rows), :] = other[slot, which]

    loop(RING, one)


def fetch(refs, held, sems):
    copies = [pltpu.make_async_copy(ref, held.at[i], sems.at[i]) for i, ref in enumerate(refs)]
    for copy in copies:
        copy.start()


def fetched(held, sems, i):
    pltpu.make_async_copy(held.at[i], held.at[i], sems.at[i]).wait()


def early_sums(table, x, *refs, turned):
    weights, (out, held, sems) = refs[:-3], refs[-3:]
    fetch(weights, held, sems)
    loop(EARLY, lambda i: fetched(held, sems, i))

    def tile(part):
        if turned:
            out[:, part] = sum(dot_t(x[n], held[n, part, :]) for n in range(EARLY))
        else:
            out[:, part] = sum(dot(x[n], held[n, :, part]) for n in range(EARLY))

    tile_loop(out.shape[1], tile)


def gate_up_late(table, x, gate_early, up_early, *refs):
    weights, (out, held, sems) = refs[:-3], refs[-3:]
    late = RING - EARLY
    fetch(weights, held, sems)
    loop(2 * late, lambda i: fetched(held, sems, i))

    def tile(part):
        for which, early in enumerate((gate_early, up_early)):
            more = sum(dot_t(x[EARLY + n], held[which * late + n, part, :]) for n in range(late))
            out[which, :, part] = early[:, part] + more

    tile_loop(out.shape[2], tile)


def grad_late(table, dy, early, *refs):
    downs, (out, held, sems) = refs[:-3], refs[-3:]
    late = NEAR - EARLY
    fetch(downs, held, sems)
    loop(late, lambda i: fetched(held, sems, i))

    def tile(part):
        out[:, part] = early[:, part] + sum(dot(dy[EARLY + n], held[n, :, part]) for n in range(late))

    tile_loop(out.shape[1], tile)


def grad_hidden_far(table, dy, near, far, out):
    def tile(part):
        out[:, part] = near[:, part] + dot(dy[NEAR], far[:, part])

    tile_loop(out.shape[1], tile)


def keep_and_give(table, n, block, both, keep, give):
    rows = keep.shape[1]
    both[...] = block.astype(BF16)
    keep[n] = both[pl.ds(pl.multiple_of(table[CORE] * rows, rows), rows), :]
    give[n] = both[pl.ds(pl.multiple_of((1 - table[CORE]) * rows, rows), rows), :]


def outputs_kernel(table, mine, other, early, late, far, keep, give, hidden, both):
    def tile(part):
        gate_pre = mine[0, :, part] + other[0, :, part]
        up_pre = mine[1, :, part] + other[1, :, part]
        activated = gate_pre * jax.nn.sigmoid(gate_pre)
        hidden[:, part] = (activated * up_pre).astype(BF16)

    tile_loop(hidden.shape[1], tile)
    loop(EARLY, lambda n: keep_and_give(table, n, dot_t(hidden[...], early[n]), both, keep, give))
    more = NEAR - EARLY
    loop(more, lambda n: keep_and_give(table, EARLY + n, dot_t(hidden[...], late[n]), both, keep, give))
    keep_and_give(table, NEAR, dot_t(hidden[...], far[...]), both, keep, give)


def input_grads_kernel(table, mine, other, by_gate, by_up, *refs):
    weights, (keep, give, gg, gu, both, held, sems) = refs[: 2 * RING], refs[2 * RING :]
    fetch(weights, held, sems)

    def tile(part):
        grad_hidden = mine[:, part] + other[:, part]
        gg[:, part] = (grad_hidden * by_gate[:, part]).astype(BF16)
        gu[:, part] = (grad_hidden * by_up[:, part]).astype(BF16)

    tile_loop(mine.shape[1], tile)

    def one(n):
        fetched(held, sems, 2 * n)
        fetched(held, sems, 2 * n + 1)
        keep_and_give(table, n, dot(gg[...], held[2 * n]) + dot(gu[...], held[2 * n + 1]), both, keep, give)

    loop(RING, one)


def arrange_columns(table, mine, other, out):
    def one(chip):
        place = table[PLACE + chip]
        out[2 * chip + table[CORE]] = mine[place]
        out[2 * chip + 1 - table[CORE]] = other[place]

    loop(RING, one)


def finish_kernel(table, got, done, back):
    share = done.shape[0]

    def add(j):
        part = pl.ds(pl.multiple_of(j * BLOCK, BLOCK), BLOCK)
        total = sum(got[s, part, :].astype(F32) for s in range(got.shape[0]))
        done[j] = jnp.where(table[j] != 0, total, 0.0).astype(BF16)

    def send(j):
        block = done[table[2 * share + j]].astype(F32)
        back[j] = jnp.where(table[share + j] != 0, block, 0.0).astype(BF16)

    loop(share, add)
    loop(share, send)


def per_device(tokens, cotangent, gate_weight, up_weight, down_weight, counts):
    rank = lax.axis_index("dp")
    z, c = rank // 2, rank % 2

    def around(own, hops):
        right, left = [own], [own]
        for _ in range(hops):
            right.append(ring(right[-1], 1))
            left.append(ring(left[-1], -1))
        return right, left

    g_r, g_l = around(gate_weight.T, 3)
    u_r, u_l = around(up_weight.T, 3)
    d_r, d_l = around(down_weight.T, 3)
    g_far = ring(g_r[3], 1)
    u_far = ring(u_l[3], -1)
    d_far = ring(d_l[3], -1)

    def near_of(r, l):
        slices = {0: r[0], 1: l[1], 2: l[2], 3: l[3], 5: r[3], 6: r[2], 7: r[1]}
        return [slices[k] for k in ARRIVAL[:-1]]

    rank_count = lax.axis_size("dp")
    blocks = tokens.shape[0] // BLOCK
    columns = tokens.shape[1]
    own_blocks = counts[rank]
    share = blocks // 2
    rows = share * BLOCK
    partner_count = counts[(rank + rank_count // 2) % rank_count]
    got = opposite(jnp.stack([tokens[rows:], cotangent[rows:]]))
    keep_blocks = jnp.minimum(own_blocks, share)
    slot_ids = jnp.arange(share, dtype=jnp.int32)
    foreign = slot_ids - own_blocks
    mine = slot_ids < keep_blocks
    valid = mine | (foreign >= 0) & (foreign < partner_count - share)
    source_index = jnp.where(mine, slot_ids, share + jnp.clip(foreign, 0, share - 1))
    lower = jnp.stack([tokens[:rows], cotangent[:rows]])
    stacked = jnp.concatenate([lower.reshape(2, share, BLOCK, columns), got.reshape(2, share, BLOCK, columns)], axis=1)
    pieces = jnp.take(stacked, source_index, axis=1)
    pieces = jnp.where(valid[None, :, None, None], pieces, jnp.zeros_like(pieces))
    work = pieces.reshape(2, rows, columns)

    spread = jnp.broadcast_to(work[None], (SIDE * SIDE, *work.shape))
    every = lax.all_to_all(spread, "tensor", 0, 0, tiled=True)
    slots = 2 * ((z + jnp.array(ARRIVAL, jnp.int32)) % RING) + c
    order = jnp.array([ARRIVAL.index(k) for k in range(RING)], jnp.int32)
    places = lax.dynamic_slice_in_dim(jnp.concatenate([order, order]), (RING - z) % RING, RING)
    every_other = swap(every)
    table = jnp.concatenate([c[None], slots, places]).astype(jnp.int32)
    wide = (RING, 2 * rows, columns)
    x_all, dy_all = call(arrange_features, [(wide, BF16)] * 2, table, every, every_other)

    ff = gate_weight.shape[1]
    by_row = (2 * rows, ff)

    def arrivals(count):
        return [pltpu.SemaphoreType.DMA((count,))]

    def early_of(x, slices, turned, keep=False):
        held = (EARLY, *slices[0].shape)
        return call(
            functools.partial(early_sums, turned=turned),
            [(by_row, F32)] + [(held, BF16)] * keep, table, x, loaded=slices[:EARLY],
            scratch=[pltpu.VMEM(held, BF16)] * (not keep) + arrivals(EARLY),
        )

    gate_all, up_all = near_of(g_r, g_l) + [g_far], near_of(u_r, u_l) + [u_far]
    gate_early = early_of(x_all, gate_all, True)[0]
    up_early = early_of(x_all, up_all, True)[0]
    late = RING - EARLY
    parts = call(
        gate_up_late, [((2,) + by_row, F32)], table, x_all, gate_early, up_early,
        loaded=gate_all[EARLY:] + up_all[EARLY:],
        scratch=[pltpu.VMEM((2 * late, ff, columns), BF16)] + arrivals(2 * late),
    )[0]
    parts_other = swap(parts)
    sums = parts + parts_other
    gate_pre, up_pre = sums[0], sums[1]
    sigmoid_gate = jax.nn.sigmoid(gate_pre)
    activated = gate_pre * sigmoid_gate
    by_gate = up_pre * sigmoid_gate * (1.0 + gate_pre * (1.0 - sigmoid_gate))

    eight = ((RING, rows, columns), BF16)
    both = pltpu.VMEM((2 * rows, columns), BF16)

    def reduce_columns(keep, give):
        share_of = ((2 * RING, rows, columns), BF16)
        got_cols = swap(give)
        blocks_for = call(arrange_columns, [share_of], table, keep, got_cols)[0]
        return lax.all_to_all(blocks_for, "tensor", 0, 0, tiled=True)

    down_near = near_of(d_r, d_l)
    grad_early, down_early = early_of(dy_all, down_near, False, keep=True)
    grad_near, down_late = call(
        grad_late, [(by_row, F32), ((NEAR - EARLY, columns, ff), BF16)], table, dy_all, grad_early,
        loaded=down_near[EARLY:], scratch=arrivals(NEAR - EARLY),
    )
    grad_part = call(grad_hidden_far, [(by_row, F32)], table, dy_all, grad_near, d_far)[0]
    grad_other = swap(grad_part)
    out = call(
        outputs_kernel, [eight, eight], table, parts, parts_other, down_early, down_late, d_far,
        scratch=[pltpu.VMEM(by_row, BF16), both],
    )
    out_sum = reduce_columns(*out)
    pairs = zip(near_of(g_r, g_l) + [g_far], near_of(u_r, u_l) + [u_far])
    dx_weights = [w for pair in pairs for w in pair]
    scratch = [pltpu.VMEM(by_row, BF16)] * 2 + [both, pltpu.VMEM((2 * RING, ff, columns), BF16)] + arrivals(2 * RING)
    dx = call(
        input_grads_kernel, [eight, eight], table, grad_part, grad_other, by_gate, activated,
        loaded=dx_weights, scratch=scratch,
    )
    dx_sum = reduce_columns(*dx)

    back_pos = own_blocks + slot_ids
    back_ok = back_pos < share
    back_index = jnp.clip(back_pos, 0, share - 1)
    upper_live = slot_ids < own_blocks - share

    blocks_table = jnp.concatenate([valid, back_ok, back_index]).astype(jnp.int32)

    def home(got_blocks):
        eight_blocks = ((share, BLOCK, columns), BF16)
        done, back = call(finish_kernel, [eight_blocks] * 2, blocks_table, got_blocks)
        returned = opposite(back)
        low = jnp.where(mine[:, None, None], done, jnp.zeros_like(done))
        high = jnp.where(upper_live[:, None, None], returned, jnp.zeros_like(returned))
        return jnp.concatenate([low, high], axis=0).reshape(2 * rows, columns)

    return home(out_sum), home(dx_sum)


def solution(mesh):
    in_specs = (
        P("dp", "tensor"),
        P("dp", "tensor"),
        P("dp", "tensor"),
        P("dp", "tensor"),
        P("tensor", "dp"),
        P(),
    )
    out_specs = (P("dp", "tensor"), P("dp", "tensor"))

    return jax.shard_map(per_device, mesh=mesh, in_specs=in_specs, out_specs=out_specs, check_vma=False)
```
